256 devices in a mesh: rep: 1, dp: 256 (over x, y, z, core).
Axes of the slice: x: 4, y: 4, z: 8, core: 2. Of those that a mesh axis runs over, the one named last changes fastest.
Arguments:
- a: bfloat16 [256, 2, 2048, 1024], P(('rep', 'dp'))
- g: bfloat16 [256, 2, 2048, 2816], P(('rep', 'dp'))
Outputs:
- output: bfloat16 [2, 1024, 2816], P('rep')
All inputs are finite; a program needn't handle non-finite values.
Results may differ from the reference program's by a relative error of at most 0.012.
Values are sent between devices in bfloat16 or wider.
A program may use at most 768 MiB of HBM per device.

```python
import jax
import jax.numpy as jnp
from jax import lax

DEVICES = 256
MATRICES = 2
TOKENS = 2048
D = 1024
FF = 2816


def setup_inputs(seed: int = 0, part: int = 0) -> dict:
    ka, kg, ks = (jax.random.fold_in(k, part) for k in jax.random.split(jax.random.key(seed), 3))
    size = 2.0 ** jax.random.uniform(ks, (DEVICES, MATRICES, 1, 1), jnp.float32, -1.0, 1.0)
    a = jax.random.normal(ka, (DEVICES, MATRICES, TOKENS, D), jnp.float32)
    g = size * jax.random.normal(kg, (DEVICES, MATRICES, TOKENS, FF), jnp.float32) * (DEVICES * TOKENS) ** -0.5
    return {"a": a.astype(jnp.bfloat16), "g": g.astype(jnp.bfloat16)}


def reference(a, g):
    def take(so_far, one):
        term = jnp.einsum("ntd,ntf->ndf", *one, preferred_element_type=jnp.float32).astype(jnp.bfloat16)
        return so_far + term.astype(jnp.float32), None

    return lax.scan(take, jnp.zeros((MATRICES, D, FF), jnp.float32), (a, g))[0].astype(jnp.bfloat16)
```

```python
import jax
import jax.numpy as jnp
from jax import lax
from jax.experimental import pallas as pl
from jax.experimental.pallas import tpu as pltpu
from jax.sharding import PartitionSpec as P

BF16, F32 = jnp.bfloat16, jnp.float32
COLS = 256
LANES = 128
HALVE = {1: 3, 2: 5, 3: 7, 4: 9, 5: 11}
SWAP, SUM = 13, 16
GATHER = {4: 18, 3: 20, 2: 22, 1: 24, 0: 26}
DONE = 29


def kernel(
    blocks,
    a_ref,
    g_ref,
    out_ref,
    a_buf,
    g_buf,
    term,
    p_out,
    p_in,
    keep,
    st0, st1, st2, st3, st4, st5,
    rv0, rv1, rv2, rv3, rv4, rv5,
    x_out,
    x_in,
    a_sem,
    g_sem,
    p_send,
    p_recv,
    send,
    recv,
):
    stage, inbox = (st0, st1, st2, st3, st4, st5), (rv0, rv1, rv2, rv3, rv4, rv5)
    units = 2 * blocks
    rows = out_ref.shape[1]
    me = lax.axis_index("dp")
    core, z, y, x = me % 2, (me // 2) % 8, (me // 16) % 4, me // 64
    mate = me + 1 - 2 * core
    far = me + (((z + 4) % 8) - z) * 2

    def even(v):
        return 1 - 2 * (v % 2)

    def odd(v, n):
        return ((v + n - even(v)) % n) - v

    links = (
        me + 64 * even(x),
        me + 16 * even(y),
        me + 2 * even(z),
        me + 64 * odd(x, 4),
        me + 16 * odd(y, 4),
        me + 2 * odd(z, 8),
    )
    bits = (
        ((x + 1) // 2) % 2,
        ((y + 1) // 2) % 2,
        ((z + 1) // 2) % 2,
        (x // 2) % 2,
        (y // 2) % 2,
        (z // 2) % 2,
    )

    def pick(k, values):
        found = values[5]
        for i in range(5):
            found = jnp.where(k == i, values[i], found)
        return found

    def load_a(i):
        n = (core + 1 + i) % 2
        return pltpu.make_async_copy(a_ref.at[0, n], a_buf.at[i], a_sem.at[i])

    def load_g(i):
        own = jnp.where(i == 0, 0, (i + 1) % 2)
        own = jnp.where(i == 2 * blocks - 1, 1, own)
        block = jnp.where(own == 1, i // 2 - 1 + (i // (2 * blocks - 1)), (i + 1) // 2)
        n = (core + 1 + own) % 2
        col = pl.multiple_of(block * COLS, COLS)
        return pltpu.make_async_copy(
            g_ref.at[0, n, :, pl.ds(col, COLS)], g_buf.at[i % 4], g_sem.at[i % 4]
        )

    def multiply(i, which):
        load_g(i).wait()

        @pl.when(i + 3 < 2 * blocks)
        def _():
            load_g(i + 3).start()

        return lax.dot_general(
            a_buf[which],
            g_buf[i % 4],
            (((0,), (0,)), ((), ())),
            preferred_element_type=F32,
        )

    def push(src, dst, s_sem, r_sem, to):
        return pltpu.make_async_remote_copy(
            src_ref=src,
            dst_ref=dst,
            send_sem=s_sem,
            recv_sem=r_sem,
            device_id={"dp": to},
            device_id_type=pl.DeviceIdType.MESH,
        )

    def push_mate(b):
        return push(p_out.at[b], p_in.at[b], p_send.at[b], p_recv.at[b], mate)

    def push_half(u, s):
        return push(
            stage[s].at[u],
            inbox[s].at[u],
            send.at[s, u],
            recv.at[s, u],
            pick((u + s) % 6, links),
        )

    def push_far(u):
        return push(x_out.at[u], x_in.at[u], send.at[6, u], recv.at[6, u], far)

    def kept(u, s):
        begin = 0
        for k in range(s):
            begin = begin + pick((u + k) % 6, bits) * (rows >> (k + 1))
        return begin

    def push_rows(u, s, begin, to, slot):
        place = out_ref.at[
            core,
            pl.ds(pl.multiple_of(begin, 16), rows >> (s + 1)),
            pl.ds(pl.multiple_of(u * LANES, LANES), LANES),
        ]
        return push(place, place, send.at[slot, u], recv.at[slot, u], to)

    def push_gather(u, s):
        return push_rows(u, s, kept(u, s + 1), pick((u + s) % 6, links), 7 + s)

    def wait_gather(u, s):
        bit = pick((u + s) % 6, bits)
        begin = kept(u, s) + (1 - bit) * (rows >> (s + 1))
        push_rows(u, s, begin, pick((u + s) % 6, links), 7 + s).wait_recv()

    def push_done(u, owner):
        place = out_ref.at[owner, :, pl.ds(pl.multiple_of(u * LANES, LANES), LANES)]
        return push(place, place, send.at[13, u], recv.at[13, u], mate)

    def each(begin, count, size, fn):
        step = min(size, count)
        for i in range(count // step):
            fn(pl.ds(pl.multiple_of(begin + i * step, 16), step), pl.ds(i * step, step))

    for i in range(2):
        load_a(i).start()
    for i in range(3):
        load_g(i).start()

    barrier = pltpu.get_barrier_semaphore()
    for other in (*links, far, mate):
        pl.semaphore_signal(
            barrier,
            inc=1,
            device_id={"dp": other},
            device_id_type=pl.DeviceIdType.MESH,
        )

    def mate_block(b, i):
        p_out[b] = multiply(i, 0).astype(BF16)
        push_mate(b).start()

    load_a(0).wait()
    load_a(1).wait()
    pl.semaphore_wait(barrier, 8)
    mate_block(0, 0)

    def first_half(u, h):
        bit = pick(u % 6, bits)
        cols = slice(h * LANES, (h + 1) * LANES)
        half = rows // 2

        def to_send(src, dst):
            both = term[src, cols] + p_in[u // 2, src, cols].astype(F32)
            st0[u, dst, :] = both.astype(BF16)

        def to_keep(src, dst):
            keep[u, dst, :] = term[src, cols] + p_in[u // 2, src, cols].astype(F32)

        each((1 - bit) * half, half, 128, to_send)
        push_half(u, 0).start()
        each(bit * half, half, 128, to_keep)

    def halve(u, s):
        size = rows >> (s + 1)
        bit = pick((u + s) % 6, bits)
        base = kept(u, s) - kept(u, 1)
        push_half(u, s - 1).wait_recv()
        gone, stay = (1 - bit) * size, bit * size

        def at(begin, i, n):
            return pl.ds(pl.multiple_of(begin + i, 16), n)

        n = min(size, 128)
        for i in range(0, size, n):
            both = keep[u, at(base + gone, i, n), :] + inbox[s - 1][
                u, at(gone, i, n), :
            ].astype(F32)
            stage[s][u, pl.ds(i, n), :] = both.astype(BF16)
        push_half(u, s).start()
        for i in range(0, size, n):
            keep[u, at(base + stay, i, n), :] = keep[
                u, at(base + stay, i, n), :
            ] + inbox[s - 1][u, at(stay, i, n), :].astype(F32)

    def swap(u):
        push_half(u, 5).wait_recv()
        at = pl.ds(pl.multiple_of(kept(u, 6) - kept(u, 1), 16), 16)
        x_out[u] = (keep[u, at, :] + rv5[u].astype(F32)).astype(BF16)
        push_far(u).start()

    def total(u):
        push_far(u).wait_recv()
        both = (x_out[u].astype(F32) + x_in[u].astype(F32)).astype(BF16)
        at = pl.ds(pl.multiple_of(kept(u, 6), 16), 16)
        out_ref[core, at, pl.ds(pl.multiple_of(u * LANES, LANES), LANES)] = both
        push_gather(u, 5).start()

    def gather(u, s):
        wait_gather(u, s + 1)
        push_gather(u, s).start()

    def done(u):
        wait_gather(u, 0)
        push_done(u, core).start()

    def slot(t, _):
        @pl.when(t < blocks)
        def _():
            @pl.when(t + 1 < blocks)
            def _():
                mate_block(t + 1, 2 * t + 1)

            term[...] = multiply(jnp.where(t == blocks - 1, 2 * t + 1, 2 * t + 2), 1)
            push_mate(t).wait_recv()
            for h in range(2):
                first_half(2 * t + h, h)

        def late(delay, fn):
            b = t - delay

            @pl.when((b >= 0) & (b < blocks))
            def _():
                def one(h, _):
                    fn(2 * b + h)
                    return 0

                lax.fori_loop(0, 2, one, 0)

        late(DONE, done)
        for s in range(5):
            late(GATHER[s], lambda u, s=s: gather(u, s))
        late(SUM, total)
        late(SWAP, swap)
        for s in range(5, 0, -1):
            late(HALVE[s], lambda u, s=s: halve(u, s))
        return 0

    lax.fori_loop(0, blocks + DONE, slot, 0)

    def finish_block(b, _):
        push_mate(b).wait_send()
        return 0

    lax.fori_loop(0, blocks, finish_block, 0)

    def finish(u, _):
        for s in range(6):
            push_half(u, s).wait_send()
            push_gather(u, s).wait_send()
        push_far(u).wait_send()
        push_done(u, 1 - core).wait_recv()
        push_done(u, core).wait_send()
        return 0

    lax.fori_loop(0, units, finish, 0)


def solution(mesh):
    def step(a, g):
        (_, n, tokens, d), f = a.shape, g.shape[-1]
        blocks, units = f // COLS, f // LANES
        halves = [pltpu.VMEM((units, d >> (s + 1), LANES), BF16) for s in range(6)]
        dma = pltpu.SemaphoreType.DMA
        import functools

        return pl.pallas_call(
            functools.partial(kernel, blocks),
            out_shape=jax.ShapeDtypeStruct((n, d, f), BF16),
            in_specs=[pl.BlockSpec(memory_space=pl.ANY)] * 2,
            out_specs=pl.BlockSpec(memory_space=pltpu.VMEM),
            scratch_shapes=[
                pltpu.VMEM((2, tokens, d), BF16),
                pltpu.VMEM((4, tokens, COLS), BF16),
                pltpu.VMEM((d, COLS), F32),
                pltpu.VMEM((blocks, d, COLS), BF16),
                pltpu.VMEM((blocks, d, COLS), BF16),
                pltpu.VMEM((units, d // 2, LANES), F32),
                *halves,
                *halves,
                pltpu.VMEM((units, d >> 6, LANES), BF16),
                pltpu.VMEM((units, d >> 6, LANES), BF16),
                dma((2,)),
                dma((4,)),
                dma((blocks,)),
                dma((blocks,)),
                dma((14, units)),
                dma((14, units)),
            ],
            compiler_params=pltpu.CompilerParams(
                collective_id=0, has_side_effects=True, vmem_limit_bytes=62 * 2**20
            ),
            name="sums",
        )(a, g)

    return jax.shard_map(
        step,
        mesh=mesh,
        in_specs=(P(("rep", "dp")), P(("rep", "dp"))),
        out_specs=P("rep"),
        check_vma=False,
    )
```

```python
import functools

import jax
import jax.numpy as jnp
from jax import lax
from jax.experimental import pallas as pl
from jax.experimental.pallas import tpu as pltpu
from jax.sharding import PartitionSpec as P

BF16, F32 = jnp.bfloat16, jnp.float32
COLS = 256
LANES = 128
PIECE = 16
HALVE1, HALVE2, SCATTER, SWAP, SUM = 5, 8, 11, 14, 18
SPREAD, GATHER1, GATHER0, DONE = 21, 24, 27, 31


def kernel(
    blocks,
    a_ref,
    g_ref,
    out_ref,
    a_buf,
    g_buf,
    term,
    p_out,
    p_in,
    keep,
    st0,
    st1,
    st2,
    rv0,
    rv1,
    rv2,
    cube_out,
    cube_in,
    x_out,
    x_in,
    a_sem,
    g_sem,
    p_send,
    p_recv,
    send,
    recv,
):
    stage, inbox = (st0, st1, st2), (rv0, rv1, rv2)
    units = 2 * blocks
    rows = out_ref.shape[1]
    me = lax.axis_index("dp")
    core, z, y, x = me % 2, (me // 2) % 8, (me // 16) % 4, me // 64
    mate = me + 1 - 2 * core
    far = me + (((z + 4) % 8) - z) * 2

    def even(v):
        return 1 - 2 * (v % 2)

    def odd(v, n):
        return ((v + n - even(v)) % n) - v

    links = (
        me + 64 * even(x),
        me + 16 * even(y),
        me + 2 * even(z),
        me + 64 * odd(x, 4),
        me + 16 * odd(y, 4),
        me + 2 * odd(z, 8),
    )
    bits = (
        ((x + 1) // 2) % 2,
        ((y + 1) // 2) % 2,
        ((z + 1) // 2) % 2,
        (x // 2) % 2,
        (y // 2) % 2,
        (z // 2) % 2,
    )

    def pick(u, s, values):
        k = (u + 3 * core + s) % 6
        found = values[5]
        for i in range(5):
            found = jnp.where(k == i, values[i], found)
        return found

    def load_a(i):
        n = (core + 1 + i) % 2
        return pltpu.make_async_copy(a_ref.at[0, n], a_buf.at[i], a_sem.at[i])

    def load_g(i):
        own = jnp.where(i == 0, 0, (i + 1) % 2)
        own = jnp.where(i == 2 * blocks - 1, 1, own)
        block = jnp.where(own == 1, i // 2 - 1 + (i // (2 * blocks - 1)), (i + 1) // 2)
        n = (core + 1 + own) % 2
        col = pl.multiple_of(block * COLS, COLS)
        return pltpu.make_async_copy(
            g_ref.at[0, n, :, pl.ds(col, COLS)], g_buf.at[i % 4], g_sem.at[i % 4]
        )

    def multiply(i, which):
        load_g(i).wait()

        @pl.when(i + 3 < 2 * blocks)
        def _():
            load_g(i + 3).start()

        return lax.dot_general(
            a_buf[which],
            g_buf[i % 4],
            (((0,), (0,)), ((), ())),
            preferred_element_type=F32,
        )

    def push(src, dst, s_sem, r_sem, to):
        return pltpu.make_async_remote_copy(
            src_ref=src,
            dst_ref=dst,
            send_sem=s_sem,
            recv_sem=r_sem,
            device_id={"dp": to},
            device_id_type=pl.DeviceIdType.MESH,
        )

    def push_mate(b):
        return push(p_out.at[b], p_in.at[b], p_send.at[b], p_recv.at[b], mate)

    def push_half(u, s):
        return push(
            stage[s].at[u],
            inbox[s].at[u],
            send.at[s, u],
            recv.at[s, u],
            pick(u, s, links),
        )

    def push_far(u):
        return push(x_out.at[u], x_in.at[u], send.at[4, u], recv.at[4, u], far)

    def cube(u):
        others = []
        for m in range(1, 8):
            piece, to = 0, me
            for k in range(3):
                bit = pick(u, 3 + k, bits)
                if m >> k & 1:
                    bit = 1 - bit
                    to = to + pick(u, 3 + k, links) - me
                piece = piece + bit * ((4 * PIECE) >> k)
            others.append((m - 1, pl.multiple_of(piece, PIECE), to))
        return others

    def push_cube(u, m, piece, to):
        return push(
            cube_out.at[u, pl.ds(piece, PIECE)],
            cube_in.at[u, m],
            send.at[3, u],
            recv.at[3, u],
            to,
        )

    def all_cube(u, k):
        return push(cube_in.at[u], cube_in.at[u], send.at[k, u], recv.at[k, u], far)

    def kept(u, s):
        begin = 0
        for k in range(s):
            begin = begin + pick(u, k, bits) * (rows >> (k + 1))
        return begin

    def push_rows(u, begin, size, to, k):
        place = out_ref.at[
            core,
            pl.ds(pl.multiple_of(begin, PIECE), size),
            pl.ds(pl.multiple_of(u * LANES, LANES), LANES),
        ]
        return push(place, place, send.at[k, u], recv.at[k, u], to)

    def push_gather(u, s):
        return push_rows(u, kept(u, s + 1), rows >> (s + 1), pick(u, s, links), 6 + s)

    def wait_gather(u, s):
        begin = kept(u, s) + (1 - pick(u, s, bits)) * (rows >> (s + 1))
        push_rows(u, begin, rows >> (s + 1), pick(u, s, links), 6 + s).wait_recv()

    def push_done(u, owner):
        place = out_ref.at[owner, :, pl.ds(pl.multiple_of(u * LANES, LANES), LANES)]
        return push(place, place, send.at[9, u], recv.at[9, u], mate)

    def each(begin, count, size, fn):
        step = min(size, count)
        for i in range(count // step):
            fn(pl.ds(pl.multiple_of(begin + i * step, 16), step), pl.ds(i * step, step))

    load_a(0).start()
    load_g(0).start()
    load_g(1).start()

    barrier = pltpu.get_barrier_semaphore()
    peers = sorted(
        {
            tuple(sorted((r + 3 + k) % 6 for k in range(3) if m >> k & 1))
            for r in range(6)
            for m in range(1, 8)
        }
    )
    others = [me + sum(links[k] - me for k in peer) for peer in peers] + [far, mate]
    for other in others:
        pl.semaphore_signal(
            barrier,
            inc=1,
            device_id={"dp": other},
            device_id_type=pl.DeviceIdType.MESH,
        )

    def mate_block(b, i):
        p_out[b] = multiply(i, 0).astype(BF16)
        push_mate(b).start()

    load_a(0).wait()
    load_a(1).start()
    load_g(2).start()
    p_out[0] = multiply(0, 0).astype(BF16)
    pl.semaphore_wait(barrier, len(others))
    push_mate(0).start()

    def first_half(u, h):
        bit = pick(u, 0, bits)
        cols = slice(h * LANES, (h + 1) * LANES)
        half = rows // 2

        def to_send(src, dst):
            both = term[src, cols] + p_in[u // 2, src, cols].astype(F32)
            st0[u, dst, :] = both.astype(BF16)

        def to_keep(src, dst):
            keep[u, dst, :] = term[src, cols] + p_in[u // 2, src, cols].astype(F32)

        each((1 - bit) * half, half, 128, to_send)
        push_half(u, 0).start()
        each(bit * half, half, 128, to_keep)

    def halve(u, s):
        size = rows >> (s + 1)
        bit = pick(u, s, bits)
        base = kept(u, s) - kept(u, 1)
        push_half(u, s - 1).wait_recv()
        gone, stay = (1 - bit) * size, bit * size

        def at(begin, i, n):
            return pl.ds(pl.multiple_of(begin + i, 16), n)

        n = min(size, 128)
        for i in range(0, size, n):
            both = keep[u, at(base + gone, i, n), :] + inbox[s - 1][
                u, at(gone, i, n), :
            ].astype(F32)
            stage[s][u, pl.ds(i, n), :] = both.astype(BF16)
        push_half(u, s).start()
        for i in range(0, size, n):
            keep[u, at(base + stay, i, n), :] = keep[
                u, at(base + stay, i, n), :
            ] + inbox[s - 1][u, at(stay, i, n), :].astype(F32)

    def scatter(u):
        push_half(u, 2).wait_recv()
        base = kept(u, 3) - kept(u, 1)
        at = pl.ds(pl.multiple_of(base, PIECE), 8 * PIECE)
        both = keep[u, at, :] + rv2[u].astype(F32)
        cube_out[u] = both.astype(BF16)
        for m, piece, to in cube(u):
            push_cube(u, m, piece, to).start()
        keep[u, at, :] = both

    def swap(u):
        all_cube(u, 3).wait_recv()
        both = keep[u, pl.ds(pl.multiple_of(kept(u, 6) - kept(u, 1), PIECE), PIECE), :]
        for m in range(7):
            both = both + cube_in[u, m].astype(F32)
        x_out[u] = both.astype(BF16)
        push_far(u).start()

    def total(u):
        push_far(u).wait_recv()
        both = (x_out[u].astype(F32) + x_in[u].astype(F32)).astype(BF16)
        begin = kept(u, 6)
        at = pl.ds(pl.multiple_of(begin, PIECE), PIECE)
        out_ref[core, at, pl.ds(pl.multiple_of(u * LANES, LANES), LANES)] = both
        for _, _, to in cube(u):
            push_rows(u, begin, PIECE, to, 5).start()

    def spread(u):
        all_cube(u, 5).wait_recv()
        push_gather(u, 2).start()

    def gather(u, s):
        wait_gather(u, s + 1)
        push_gather(u, s).start()

    def done(u):
        wait_gather(u, 0)
        push_done(u, core).start()

    steps = (
        (DONE, done),
        (GATHER0, lambda u: gather(u, 0)),
        (GATHER1, lambda u: gather(u, 1)),
        (SPREAD, spread),
        (SUM, total),
        (SWAP, swap),
        (SCATTER, scatter),
        (HALVE2, lambda u: halve(u, 2)),
        (HALVE1, lambda u: halve(u, 1)),
    )

    def tick(t, part):
        for delay, fn in steps:
            if delay % 2 != part:
                continue
            b = t - delay // 2

            @pl.when((b >= 0) & (b < blocks))
            def _(b=b, fn=fn):
                def one(h, _):
                    fn(2 * b + h)
                    return 0

                lax.fori_loop(0, 2, one, 0)

    def slot(t, _):
        @pl.when(t + 1 < blocks)
        def _():
            mate_block(t + 1, 2 * t + 1)

        tick(t, 0)

        @pl.when(t < blocks)
        def _():
            @pl.when(t == 0)
            def _():
                load_a(1).wait()

            term[...] = multiply(jnp.where(t == blocks - 1, 2 * t + 1, 2 * t + 2), 1)
            push_mate(t).wait_recv()
            for h in range(2):
                first_half(2 * t + h, h)

        tick(t, 1)
        return 0

    lax.fori_loop(0, blocks + DONE // 2, slot, 0)

    def finish_block(b, _):
        push_mate(b).wait_send()
        return 0

    lax.fori_loop(0, blocks, finish_block, 0)

    def finish(u, _):
        for s in range(3):
            push_half(u, s).wait_send()
            push_gather(u, s).wait_send()
        all_cube(u, 3).wait_send()
        all_cube(u, 5).wait_send()
        push_far(u).wait_send()
        push_done(u, 1 - core).wait_recv()
        push_done(u, core).wait_send()
        return 0

    lax.fori_loop(0, units, finish, 0)


def flush(sums_ref, out_ref, sem):
    n, rows, _ = sums_ref.shape
    step = rows // 4
    copies = [
        pltpu.make_async_copy(
            sums_ref.at[i, pl.ds(j * step, step)],
            out_ref.at[i, pl.ds(j * step, step)],
            sem.at[i, j],
        )
        for i in range(n)
        for j in range(4)
    ]
    for copy in copies:
        copy.start()
    for copy in copies:
        copy.wait()


def solution(mesh):
    def step(a, g):
        (_, n, tokens, d), f = a.shape, g.shape[-1]
        blocks, units = f // COLS, f // LANES
        halves = [pltpu.VMEM((units, d >> (s + 1), LANES), BF16) for s in range(3)]
        dma = pltpu.SemaphoreType.DMA
        sums = pl.pallas_call(
            functools.partial(kernel, blocks),
            out_shape=pltpu.VMEM((n, d, f), BF16),
            in_specs=[pl.BlockSpec(memory_space=pl.ANY)] * 2,
            out_specs=pl.BlockSpec(memory_space=pltpu.VMEM),
            scratch_shapes=[
                pltpu.VMEM((2, tokens, d), BF16),
                pltpu.VMEM((4, tokens, COLS), BF16),
                pltpu.VMEM((d, COLS), F32),
                pltpu.VMEM((blocks, d, COLS), BF16),
                pltpu.VMEM((blocks, d, COLS), BF16),
                pltpu.VMEM((units, d // 2, LANES), F32),
                *halves,
                *halves,
                pltpu.VMEM((units, 8 * PIECE, LANES), BF16),
                pltpu.VMEM((units, 7, PIECE, LANES), BF16),
                pltpu.VMEM((units, PIECE, LANES), BF16),
                pltpu.VMEM((units, PIECE, LANES), BF16),
                dma((2,)),
                dma((4,)),
                dma((blocks,)),
                dma((blocks,)),
                dma((10, units)),
                dma((10, units)),
            ],
            compiler_params=pltpu.CompilerParams(
                collective_id=0, has_side_effects=True, vmem_limit_bytes=46 * 2**20
            ),
            name="sums",
        )(a, g)
        return pl.pallas_call(
            flush,
            out_shape=jax.ShapeDtypeStruct((n, d, f), BF16),
            in_specs=[pl.BlockSpec(memory_space=pltpu.VMEM)],
            out_specs=pl.BlockSpec(memory_space=pl.ANY),
            scratch_shapes=[dma((2, 4))],
            compiler_params=pltpu.CompilerParams(vmem_limit_bytes=2**20),
            name="flush",
        )(sums)

    return jax.shard_map(
        step,
        mesh=mesh,
        in_specs=(P(("rep", "dp")), P(("rep", "dp"))),
        out_specs=P("rep"),
        check_vma=False,
    )
```

```python
import functools

import jax
import jax.numpy as jnp
from jax import lax
from jax.experimental import pallas as pl
from jax.experimental.pallas import tpu as pltpu
from jax.sharding import PartitionSpec as P

BF16, F32 = jnp.bfloat16, jnp.float32
COLS = 256
LANES = 128
PIECE = 16
HALVE1, HALVE2, SCATTER, SWAP, SUM = 4, 7, 11, 15, 21
SPREAD, GATHER1, GATHER0, DONE = 26, 31, 37, 45


def kernel(
    blocks,
    a_ref,
    g_ref,
    out_ref,
    a_buf,
    g_buf,
    term,
    p_out,
    p_in,
    keep,
    st0,
    st1,
    st2,
    rv0,
    rv1,
    rv2,
    cube_out,
    cube_in,
    x_out,
    x_in,
    a_sem,
    g_sem,
    p_send,
    p_recv,
    send,
    recv,
    done_recv,
):
    stage, inbox = (st0, st1, st2), (rv0, rv1, rv2)
    rows = out_ref.shape[1]
    me = lax.axis_index("dp")
    core, z, y, x = me % 2, (me // 2) % 8, (me // 16) % 4, me // 64
    mate = me + 1 - 2 * core
    far = me + (((z + 4) % 8) - z) * 2

    def even(v):
        return 1 - 2 * (v % 2)

    def odd(v, n):
        return ((v + n - even(v)) % n) - v

    links = (
        me + 64 * even(x),
        me + 16 * even(y),
        me + 2 * even(z),
        me + 64 * odd(x, 4),
        me + 16 * odd(y, 4),
        me + 2 * odd(z, 8),
    )
    bits = (
        ((x + 1) // 2) % 2,
        ((y + 1) // 2) % 2,
        ((z + 1) // 2) % 2,
        (x // 2) % 2,
        (y // 2) % 2,
        (z // 2) % 2,
    )

    def pick(u, s, values):
        k = (u + 3 * core + s) % 6
        found = values[5]
        for i in range(5):
            found = jnp.where(k == i, values[i], found)
        return found

    def load_a(i):
        n = (core + 1 + i) % 2
        return pltpu.make_async_copy(a_ref.at[0, n], a_buf.at[i], a_sem.at[i])

    def load_g(i):
        own = jnp.where(i == 0, 0, (i + 1) % 2)
        own = jnp.where(i == 2 * blocks - 1, 1, own)
        block = jnp.where(own == 1, i // 2 - 1 + (i // (2 * blocks - 1)), (i + 1) // 2)
        n = (core + 1 + own) % 2
        col = pl.multiple_of(block * COLS, COLS)
        return pltpu.make_async_copy(
            g_ref.at[0, n, :, pl.ds(col, COLS)], g_buf.at[i % 4], g_sem.at[i % 4]
        )

    def multiply(i, which):
        load_g(i).wait()

        @pl.when(i + 3 < 2 * blocks)
        def _():
            load_g(i + 3).start()

        return lax.dot_general(
            a_buf[which],
            g_buf[i % 4],
            (((0,), (0,)), ((), ())),
            preferred_element_type=F32,
        )

    def push(src, dst, s_sem, r_sem, to):
        return pltpu.make_async_remote_copy(
            src_ref=src,
            dst_ref=dst,
            send_sem=s_sem,
            recv_sem=r_sem,
            device_id={"dp": to},
            device_id_type=pl.DeviceIdType.MESH,
        )

    def push_mate(b):
        return push(p_out.at[b], p_in.at[b], p_send, p_recv.at[b], mate)

    def push_half(u, s):
        return push(
            stage[s].at[u],
            inbox[s].at[u],
            send.at[s],
            recv.at[s, u],
            pick(u, s, links),
        )

    def push_far(u):
        return push(x_out.at[u], x_in.at[u], send.at[4], recv.at[4, u], far)

    def cube(u):
        others = []
        bit = [pick(u, 3 + k, bits) for k in range(3)]
        hop = [pick(u, 3 + k, links) - me for k in range(3)]
        for m in range(1, 8):
            piece, to = 0, me
            for k in range(3):
                there = 1 - bit[k] if m >> k & 1 else bit[k]
                piece = piece + there * ((4 * PIECE) >> k)
                to = to + hop[k] if m >> k & 1 else to
            others.append((m - 1, pl.multiple_of(piece, PIECE), to))
        return others

    def push_cube(u, m, piece, to):
        return push(
            cube_out.at[u, pl.ds(piece, PIECE)],
            cube_in.at[u, m],
            send.at[3],
            recv.at[3, u],
            to,
        )

    def arrived(u, k):
        buf = (rv0, rv1, rv2, cube_in, x_in, cube_in, rv2, rv1, rv0)[k]
        push(buf.at[u], buf.at[u], send.at[k], recv.at[k, u], mate).wait_recv()

    def kept(u, s):
        begin = 0
        for k in range(s):
            begin = begin + pick(u, k, bits) * (rows >> (k + 1))
        return begin

    def push_rows(u, begin, size, to, k):
        place = out_ref.at[
            core,
            pl.ds(pl.multiple_of(begin, PIECE), size),
            pl.ds(pl.multiple_of(u * LANES, LANES), LANES),
        ]
        return push(place, place, send.at[k], recv.at[k, u], to)

    def push_gather(u, s, begin, size):
        return push_rows(u, begin, size, pick(u, s, links), 8 - s)

    def push_done(b):
        place = out_ref.at[core, :, pl.ds(pl.multiple_of(b * COLS, COLS), COLS)]
        return push(place, place, send.at[9], done_recv, mate)

    def each(begin, count, size, fn):
        step = min(size, count)
        for i in range(count // step):
            fn(pl.ds(pl.multiple_of(begin + i * step, 16), step), pl.ds(i * step, step))

    load_a(0).start()
    load_g(0).start()
    load_g(1).start()

    barrier = pltpu.get_barrier_semaphore()
    peers = sorted(
        {
            tuple(sorted((r + 3 + k) % 6 for k in range(3) if m >> k & 1))
            for r in range(6)
            for m in range(1, 8)
        }
    )
    others = [me + sum(links[k] - me for k in peer) for peer in peers] + [far, mate]
    for other in others:
        pl.semaphore_signal(
            barrier,
            inc=1,
            device_id={"dp": other},
            device_id_type=pl.DeviceIdType.MESH,
        )

    def mate_block(b, i):
        p_out[b] = multiply(i, 0).astype(BF16)
        push_mate(b).start()

    load_a(0).wait()
    load_a(1).start()
    load_g(2).start()
    p_out[0] = multiply(0, 0).astype(BF16)
    pl.semaphore_wait(barrier, len(others))
    push_mate(0).start()

    def first_half(u, h):
        bit = pick(u, 0, bits)
        cols = slice(h * LANES, (h + 1) * LANES)
        half = rows // 2

        def to_send(src, dst):
            both = term[src, cols] + p_in[u // 2, src, cols].astype(F32)
            st0[u, dst, :] = both.astype(BF16)

        def to_keep(src, dst):
            keep[u, dst, :] = term[src, cols] + p_in[u // 2, src, cols].astype(F32)

        each((1 - bit) * half, half, 128, to_send)
        push_half(u, 0).start()
        each(bit * half, half, 128, to_keep)

    def halve(u, s):
        size = rows >> (s + 1)
        bit = pick(u, s, bits)
        base = kept(u, s) - kept(u, 1)
        gone, stay = (1 - bit) * size, bit * size

        def at(begin, i, n):
            return pl.ds(pl.multiple_of(begin + i, 16), n)

        n = min(size, 128)
        for i in range(0, size, n):
            both = keep[u, at(base + gone, i, n), :] + inbox[s - 1][
                u, at(gone, i, n), :
            ].astype(F32)
            stage[s][u, pl.ds(i, n), :] = both.astype(BF16)
        push_half(u, s).start()
        for i in range(0, size, n):
            keep[u, at(base + stay, i, n), :] = keep[
                u, at(base + stay, i, n), :
            ] + inbox[s - 1][u, at(stay, i, n), :].astype(F32)

    def scatter(u):
        base = kept(u, 3) - kept(u, 1)
        at = pl.ds(pl.multiple_of(base, PIECE), 8 * PIECE)
        both = keep[u, at, :] + rv2[u].astype(F32)
        cube_out[u] = both.astype(BF16)
        for m, piece, to in cube(u):
            push_cube(u, m, piece, to).start()
        keep[u, at, :] = both

    def swap(u):
        both = keep[u, pl.ds(pl.multiple_of(kept(u, 6) - kept(u, 1), PIECE), PIECE), :]
        for m in range(7):
            both = both + cube_in[u, m].astype(F32)
        x_out[u] = both.astype(BF16)
        push_far(u).start()

    def total(u):
        both = (x_out[u].astype(F32) + x_in[u].astype(F32)).astype(BF16)
        begin = kept(u, 6)
        at = pl.ds(pl.multiple_of(begin, PIECE), PIECE)
        out_ref[core, at, pl.ds(pl.multiple_of(u * LANES, LANES), LANES)] = both
        for _, _, to in cube(u):
            push_rows(u, begin, PIECE, to, 5).start()

    def spread(u):
        begin = kept(u, 3)
        for s in (2, 1, 0):
            push_gather(u, s, begin, rows >> 3).start()

    def gather(u, s):
        begin = kept(u, s + 1) + (1 - pick(u, s + 1, bits)) * (rows >> (s + 2))
        for k in range(s, -1, -1):
            push_gather(u, k, begin, rows >> (s + 2)).start()

    steps = (
        (HALVE1, lambda u: halve(u, 1)),
        (HALVE2, lambda u: halve(u, 2)),
        (SCATTER, scatter),
        (SWAP, swap),
        (SUM, total),
        (SPREAD, spread),
        (GATHER1, lambda u: gather(u, 1)),
        (GATHER0, lambda u: gather(u, 0)),
        (DONE, None),
    )

    def tick(t, part):
        for k, (delay, fn) in enumerate(steps):
            if delay % 2 != part:
                continue
            b = t - delay // 2

            @pl.when((b >= 0) & (b < blocks))
            def _(b=b, k=k, fn=fn):
                for h in range(2):
                    arrived(2 * b + h, k)
                    if fn is not None:
                        fn(2 * b + h)
                if fn is None:
                    push_done(b).start()

    def slot(t, _):
        @pl.when(t + 1 < blocks)
        def _():
            mate_block(t + 1, 2 * t + 1)

        tick(t, 0)

        @pl.when(t < blocks)
        def _():
            @pl.when(t == 0)
            def _():
                load_a(1).wait()

            term[...] = multiply(jnp.where(t == blocks - 1, 2 * t + 1, 2 * t + 2), 1)
            push_mate(t).wait_recv()
            for h in range(2):
                first_half(2 * t + h, h)

        tick(t, 1)
        return 0

    lax.fori_loop(0, blocks + DONE // 2, slot, 0)

    sent = (st0, st1, st2, cube_in, x_out, cube_in, st2, st1, st0, out_ref.at[core])
    for k, all_of in enumerate(sent):
        push(all_of, all_of, send.at[k], done_recv, mate).wait_send()
    push(p_out, p_out, p_send, done_recv, mate).wait_send()
    whole = out_ref.at[1 - core]
    push(whole, whole, send.at[9], done_recv, mate).wait_recv()


def flush(sums_ref, out_ref, sem):
    n, rows, _ = sums_ref.shape
    step = rows // 4
    copies = [
        pltpu.make_async_copy(
            sums_ref.at[i, pl.ds(j * step, step)],
            out_ref.at[i, pl.ds(j * step, step)],
            sem.at[i, j],
        )
        for i in range(n)
        for j in range(4)
    ]
    for copy in copies:
        copy.start()
    for copy in copies:
        copy.wait()


def solution(mesh):
    def step(a, g):
        (_, n, tokens, d), f = a.shape, g.shape[-1]
        blocks, units = f // COLS, f // LANES
        halves = [pltpu.VMEM((units, d >> (s + 1), LANES), BF16) for s in range(3)]
        dma = pltpu.SemaphoreType.DMA
        sums = pl.pallas_call(
            functools.partial(kernel, blocks),
            out_shape=pltpu.VMEM((n, d, f), BF16),
            in_specs=[pl.BlockSpec(memory_space=pl.ANY)] * 2,
            out_specs=pl.BlockSpec(memory_space=pltpu.VMEM),
            scratch_shapes=[
                pltpu.VMEM((2, tokens, d), BF16),
                pltpu.VMEM((4, tokens, COLS), BF16),
                pltpu.VMEM((d, COLS), F32),
                pltpu.VMEM((blocks, d, COLS), BF16),
                pltpu.VMEM((blocks, d, COLS), BF16),
                pltpu.VMEM((units, d // 2, LANES), F32),
                *halves,
                *halves,
                pltpu.VMEM((units, 8 * PIECE, LANES), BF16),
                pltpu.VMEM((units, 7, PIECE, LANES), BF16),
                pltpu.VMEM((units, PIECE, LANES), BF16),
                pltpu.VMEM((units, PIECE, LANES), BF16),
                dma((2,)),
                dma((4,)),
                dma,
                dma((blocks,)),
                dma((10,)),
                dma((9, units)),
                dma,
            ],
            compiler_params=pltpu.CompilerParams(
                collective_id=0, has_side_effects=True, vmem_limit_bytes=46 * 2**20
            ),
            name="sums",
        )(a, g)
        return pl.pallas_call(
            flush,
            out_shape=jax.ShapeDtypeStruct((n, d, f), BF16),
            in_specs=[pl.BlockSpec(memory_space=pltpu.VMEM)],
            out_specs=pl.BlockSpec(memory_space=pl.ANY),
            scratch_shapes=[dma((2, 4))],
            compiler_params=pltpu.CompilerParams(vmem_limit_bytes=2**20),
            name="flush",
        )(sums)

    return jax.shard_map(
        step,
        mesh=mesh,
        in_specs=(P(("rep", "dp")), P(("rep", "dp"))),
        out_specs=P("rep"),
        check_vma=False,
    )
```

```python
import functools

import jax
import jax.numpy as jnp
from jax import lax
from jax.experimental import pallas as pl
from jax.experimental.pallas import tpu as pltpu
from jax.sharding import PartitionSpec as P

BF16, F32 = jnp.bfloat16, jnp.float32
COLS = 256
LANES = 128
PIECE = 16
HALVE1, HALVE2, SCATTER, SWAP, SUM = 5, 9, 13, 18, 24
SPREAD, GATHER1, GATHER0, DONE = 30, 35, 41, 48


def kernel(
    blocks,
    a_ref,
    g_ref,
    out_ref,
    a_buf,
    g_buf,
    term,
    p_out,
    p_in,
    keep,
    st0,
    st1,
    st2,
    rv0,
    rv1,
    rv2,
    cube_out,
    cube_in,
    x_out,
    x_in,
    a_sem,
    g_sem,
    p_send,
    p_recv,
    send,
    recv,
    done_recv,
):
    stage, inbox = (st0, st1, st2), (rv0, rv1, rv2)
    rows = out_ref.shape[1]
    me = lax.axis_index("dp")
    core, z, y, x = me % 2, (me // 2) % 8, (me // 16) % 4, me // 64
    mate = me + 1 - 2 * core
    far = me + (((z + 4) % 8) - z) * 2

    def even(v):
        return 1 - 2 * (v % 2)

    def odd(v, n):
        return ((v + n - even(v)) % n) - v

    links = (
        me + 64 * even(x),
        me + 16 * even(y),
        me + 2 * even(z),
        me + 64 * odd(x, 4),
        me + 16 * odd(y, 4),
        me + 2 * odd(z, 8),
    )
    bits = (
        ((x + 1) // 2) % 2,
        ((y + 1) // 2) % 2,
        ((z + 1) // 2) % 2,
        (x // 2) % 2,
        (y // 2) % 2,
        (z // 2) % 2,
    )

    def pick(u, s, values):
        k = (u + 3 * core + s) % 6
        found = values[5]
        for i in range(5):
            found = jnp.where(k == i, values[i], found)
        return found

    def load_a(i):
        n = (core + 1 + i) % 2
        return pltpu.make_async_copy(a_ref.at[0, n], a_buf.at[i], a_sem.at[i])

    def load_g(i):
        own = jnp.where(i == 0, 0, (i + 1) % 2)
        own = jnp.where(i == 2 * blocks - 1, 1, own)
        block = jnp.where(own == 1, i // 2 - 1 + (i // (2 * blocks - 1)), (i + 1) // 2)
        n = (core + 1 + own) % 2
        col = pl.multiple_of(block * COLS, COLS)
        return pltpu.make_async_copy(
            g_ref.at[0, n, :, pl.ds(col, COLS)], g_buf.at[i % 4], g_sem.at[i % 4]
        )

    def multiply(i, which):
        load_g(i).wait()

        @pl.when(i + 3 < 2 * blocks)
        def _():
            load_g(i + 3).start()

        return lax.dot_general(
            a_buf[which],
            g_buf[i % 4],
            (((0,), (0,)), ((), ())),
            preferred_element_type=F32,
        )

    def push(src, dst, s_sem, r_sem, to):
        return pltpu.make_async_remote_copy(
            src_ref=src,
            dst_ref=dst,
            send_sem=s_sem,
            recv_sem=r_sem,
            device_id={"dp": to},
            device_id_type=pl.DeviceIdType.MESH,
        )

    def push_mate(b):
        return push(p_out.at[b], p_in.at[b], p_send, p_recv.at[b], mate)

    def push_half(u, s):
        return push(
            stage[s].at[u],
            inbox[s].at[u],
            send.at[s],
            recv.at[s, u],
            pick(u, s, links),
        )

    def push_far(u):
        return push(x_out.at[u], x_in.at[u], send.at[4], recv.at[4, u], far)

    def cube(u):
        others = []
        bit = [pick(u, 3 + k, bits) for k in range(3)]
        hop = [pick(u, 3 + k, links) - me for k in range(3)]
        for m in range(1, 8):
            piece, to = 0, me
            for k in range(3):
                there = 1 - bit[k] if m >> k & 1 else bit[k]
                piece = piece + there * ((4 * PIECE) >> k)
                to = to + hop[k] if m >> k & 1 else to
            others.append((m - 1, pl.multiple_of(piece, PIECE), to))
        return others

    def push_cube(u, m, piece, to):
        return push(
            cube_out.at[u, pl.ds(piece, PIECE)],
            cube_in.at[u, m],
            send.at[3],
            recv.at[3, u],
            to,
        )

    def arrived(u, k):
        buf = (rv0, rv1, rv2, cube_in, x_in, cube_in, rv2, rv1, rv0)[k]
        push(buf.at[u], buf.at[u], send.at[k], recv.at[k, u], mate).wait_recv()

    def kept(u, s):
        begin = 0
        for k in range(s):
            begin = begin + pick(u, k, bits) * (rows >> (k + 1))
        return begin

    def push_rows(u, begin, size, to, k):
        place = out_ref.at[
            core,
            pl.ds(pl.multiple_of(begin, PIECE), size),
            pl.ds(pl.multiple_of(u * LANES, LANES), LANES),
        ]
        return push(place, place, send.at[k], recv.at[k, u], to)

    def push_gather(u, s, begin, size):
        return push_rows(u, begin, size, pick(u, s, links), 8 - s)

    def push_done(b):
        place = out_ref.at[core, :, pl.ds(pl.multiple_of(b * COLS, COLS), COLS)]
        return push(place, place, send.at[9], done_recv, mate)

    def each(begin, count, size, fn):
        step = min(size, count)
        for i in range(count // step):
            fn(pl.ds(pl.multiple_of(begin + i * step, 16), step), pl.ds(i * step, step))

    load_a(0).start()
    load_g(0).start()
    load_g(1).start()

    barrier = pltpu.get_barrier_semaphore()
    peers = sorted(
        {
            tuple(sorted((r + 3 + k) % 6 for k in range(3) if m >> k & 1))
            for r in range(6)
            for m in range(1, 8)
        }
    )
    others = [me + sum(links[k] - me for k in peer) for peer in peers] + [far, mate]
    for other in others:
        pl.semaphore_signal(
            barrier,
            inc=1,
            device_id={"dp": other},
            device_id_type=pl.DeviceIdType.MESH,
        )

    def mate_block(b, i):
        p_out[b] = multiply(i, 0).astype(BF16)
        push_mate(b).start()

    load_a(0).wait()
    load_a(1).start()
    load_g(2).start()
    p_out[0] = multiply(0, 0).astype(BF16)
    pl.semaphore_wait(barrier, len(others))
    push_mate(0).start()

    def first_half(u, h):
        bit = pick(u, 0, bits)
        cols = slice(h * LANES, (h + 1) * LANES)
        half = rows // 2

        def to_send(src, dst):
            both = term[src, cols] + p_in[u // 2, src, cols].astype(F32)
            st0[u, dst, :] = both.astype(BF16)

        def to_keep(src, dst):
            keep[u, dst, :] = term[src, cols] + p_in[u // 2, src, cols].astype(F32)

        each((1 - bit) * half, half, 128, to_send)
        push_half(u, 0).start()
        each(bit * half, half, 128, to_keep)

    def halve(u, s):
        size = rows >> (s + 1)
        bit = pick(u, s, bits)
        base = kept(u, s) - kept(u, 1)
        gone, stay = (1 - bit) * size, bit * size

        def at(begin, i, n):
            return pl.ds(pl.multiple_of(begin + i, 16), n)

        n = min(size, 128)
        for i in range(0, size, n):
            both = keep[u, at(base + gone, i, n), :] + inbox[s - 1][
                u, at(gone, i, n), :
            ].astype(F32)
            stage[s][u, pl.ds(i, n), :] = both.astype(BF16)
        push_half(u, s).start()
        for i in range(0, size, n):
            keep[u, at(base + stay, i, n), :] = keep[
                u, at(base + stay, i, n), :
            ] + inbox[s - 1][u, at(stay, i, n), :].astype(F32)

    def scatter(u):
        base = kept(u, 3) - kept(u, 1)
        at = pl.ds(pl.multiple_of(base, PIECE), 8 * PIECE)
        both = keep[u, at, :] + rv2[u].astype(F32)
        cube_out[u] = both.astype(BF16)
        for m, piece, to in cube(u):
            push_cube(u, m, piece, to).start()
        keep[u, at, :] = both

    def swap(u):
        both = keep[u, pl.ds(pl.multiple_of(kept(u, 6) - kept(u, 1), PIECE), PIECE), :]
        for m in range(7):
            both = both + cube_in[u, m].astype(F32)
        x_out[u] = both.astype(BF16)
        push_far(u).start()

    def total(u):
        both = (x_out[u].astype(F32) + x_in[u].astype(F32)).astype(BF16)
        begin = kept(u, 6)
        at = pl.ds(pl.multiple_of(begin, PIECE), PIECE)
        out_ref[core, at, pl.ds(pl.multiple_of(u * LANES, LANES), LANES)] = both
        for _, _, to in cube(u):
            push_rows(u, begin, PIECE, to, 5).start()

    def spread(u):
        begin = kept(u, 3)
        for s in (2, 1, 0):
            push_gather(u, s, begin, rows >> 3).start()

    def gather(u, s):
        begin = kept(u, s + 1) + (1 - pick(u, s + 1, bits)) * (rows >> (s + 2))
        for k in range(s, -1, -1):
            push_gather(u, k, begin, rows >> (s + 2)).start()

    steps = (
        (HALVE1, lambda u: halve(u, 1)),
        (HALVE2, lambda u: halve(u, 2)),
        (SCATTER, scatter),
        (SWAP, swap),
        (SUM, total),
        (SPREAD, spread),
        (GATHER1, lambda u: gather(u, 1)),
        (GATHER0, lambda u: gather(u, 0)),
        (DONE, None),
    )

    def tick(t, part):
        for k, (delay, fn) in enumerate(steps):
            if delay % 2 != part:
                continue
            b = t - delay // 2

            @pl.when((b >= 0) & (b < blocks))
            def _(b=b, k=k, fn=fn):
                def one(h, _):
                    arrived(2 * b + h, k)
                    if fn is not None:
                        fn(2 * b + h)
                    return 0

                lax.fori_loop(0, 2, one, 0)
                if fn is None:
                    push_done(b).start()

    def slot(t, _):
        @pl.when(t + 1 < blocks)
        def _():
            mate_block(t + 1, 2 * t + 1)

        tick(t, 0)

        @pl.when(t < blocks)
        def _():
            @pl.when(t == 0)
            def _():
                load_a(1).wait()

            term[...] = multiply(jnp.where(t == blocks - 1, 2 * t + 1, 2 * t + 2), 1)
            push_mate(t).wait_recv()
            for h in range(2):
                first_half(2 * t + h, h)

        tick(t, 1)
        return 0

    lax.fori_loop(0, blocks + DONE // 2, slot, 0)

    sent = (st0, st1, st2, cube_in, x_out, cube_in, st2, st1, st0, out_ref.at[core])
    for k, all_of in enumerate(sent):
        push(all_of, all_of, send.at[k], done_recv, mate).wait_send()
    push(p_out, p_out, p_send, done_recv, mate).wait_send()
    whole = out_ref.at[1 - core]
    push(whole, whole, send.at[9], done_recv, mate).wait_recv()


def flush(sums_ref, out_ref, sem):
    n, rows, _ = sums_ref.shape
    step = rows // 4
    copies = [
        pltpu.make_async_copy(
            sums_ref.at[i, pl.ds(j * step, step)],
            out_ref.at[i, pl.ds(j * step, step)],
            sem.at[i, j],
        )
        for i in range(n)
        for j in range(4)
    ]
    for copy in copies:
        copy.start()
    for copy in copies:
        copy.wait()


def solution(mesh):
    def step(a, g):
        (_, n, tokens, d), f = a.shape, g.shape[-1]
        blocks, units = f // COLS, f // LANES
        halves = [pltpu.VMEM((units, d >> (s + 1), LANES), BF16) for s in range(3)]
        dma = pltpu.SemaphoreType.DMA
        sums = pl.pallas_call(
            functools.partial(kernel, blocks),
            out_shape=pltpu.VMEM((n, d, f), BF16),
            in_specs=[pl.BlockSpec(memory_space=pl.ANY)] * 2,
            out_specs=pl.BlockSpec(memory_space=pltpu.VMEM),
            scratch_shapes=[
                pltpu.VMEM((2, tokens, d), BF16),
                pltpu.VMEM((4, tokens, COLS), BF16),
                pltpu.VMEM((d, COLS), F32),
                pltpu.VMEM((blocks, d, COLS), BF16),
                pltpu.VMEM((blocks, d, COLS), BF16),
                pltpu.VMEM((units, d // 2, LANES), F32),
                *halves,
                *halves,
                pltpu.VMEM((units, 8 * PIECE, LANES), BF16),
                pltpu.VMEM((units, 7, PIECE, LANES), BF16),
                pltpu.VMEM((units, PIECE, LANES), BF16),
                pltpu.VMEM((units, PIECE, LANES), BF16),
                dma((2,)),
                dma((4,)),
                dma,
                dma((blocks,)),
                dma((10,)),
                dma((9, units)),
                dma,
            ],
            compiler_params=pltpu.CompilerParams(
                collective_id=0, has_side_effects=True, vmem_limit_bytes=46 * 2**20
            ),
            name="sums",
        )(a, g)
        return pl.pallas_call(
            flush,
            out_shape=jax.ShapeDtypeStruct((n, d, f), BF16),
            in_specs=[pl.BlockSpec(memory_space=pltpu.VMEM)],
            out_specs=pl.BlockSpec(memory_space=pl.ANY),
            scratch_shapes=[dma((2, 4))],
            compiler_params=pltpu.CompilerParams(vmem_limit_bytes=2**20),
            name="flush",
        )(sums)

    return jax.shard_map(
        step,
        mesh=mesh,
        in_specs=(P(("rep", "dp")), P(("rep", "dp"))),
        out_specs=P("rep"),
        check_vma=False,
    )
```
